32 devices in a mesh: sa: 8 (over z, x), ka: 2 (over y), vert: 2 (over core).
Axes of the slice: x: 2, y: 2, z: 4, core: 2. Of those that a mesh axis runs over, the one named last changes fastest.
Arguments:
- queries: bfloat16 [1024, 16, 128], P('sa', None, 'ka'), may hold values from -6 to 6
- key_rows: bfloat16 [1024, 16, 128], P('sa', None, 'ka'), may hold values from -6 to 6
- values: bfloat16 [1024, 16, 256], P('sa', None, 'vert'), may hold values from -6 to 6
- log_decays: bfloat16 [1024, 16, 128], P('sa', None, 'ka'), may hold values from -2 to 0
- output_grad: bfloat16 [1024, 16, 256], P('sa', None, 'vert'), may hold values from -0.1875 to 0.1875
Outputs:
- query_grad: float32 [1024, 16, 128], P('sa', 'vert', 'ka')
- key_grad: float32 [1024, 16, 128], P('sa', 'vert', 'ka')
- value_grad: float32 [1024, 16, 256], P('sa', 'ka', 'vert')
- decay_grad: float32 [1024, 16, 128], P('sa', 'vert', 'ka')
The draws below stay inside these ranges and needn't reach their ends.
All inputs are finite; a program needn't handle non-finite values.
Results may differ from the reference program's by a relative error of at most 0.0003.
Values may be sent and summed in bfloat16 or wider, within the bound.
A program may use at most 192 MiB of HBM per device.

```python
import math
import jax
import jax.numpy as jnp
from jax import lax

HEAD_NUMBER = 16
DK = 128
DV = 256
TILE_LEN = 64
TOK_DEV = 128
TOKEN_POSITIONS = 1024


def draw_log_decays(key, part):
    draw_keys = jax.random.split(jax.random.fold_in(key, 7), 7)
    slow_share = 0.5
    is_slow = jax.random.uniform(draw_keys[0], (HEAD_NUMBER, DK)) < slow_share
    slow_rate = jnp.exp(jax.random.uniform(draw_keys[1], (HEAD_NUMBER, DK), minval=math.log(0.15), maxval=math.log(0.45))) / TOKEN_POSITIONS
    fast_rate = math.log(10.0) / jnp.exp(jax.random.uniform(draw_keys[2], (HEAD_NUMBER, DK), minval=math.log(30.0), maxval=math.log(50.0)))
    step_rate = jnp.where(is_slow, slow_rate, fast_rate)
    block_count = TOKEN_POSITIONS // TOK_DEV
    block_factor = jnp.exp(jax.random.uniform(draw_keys[3], (block_count, 1, HEAD_NUMBER, 1), minval=math.log(0.5), maxval=math.log(2.0)))
    roughness = jax.random.uniform(draw_keys[4], (block_count, TOK_DEV, HEAD_NUMBER, DK), minval=0.4, maxval=1.6)
    logarithm_decay = -(step_rate[None, None] * block_factor * roughness).reshape(TOKEN_POSITIONS, HEAD_NUMBER, DK)
    spike_locations = jax.random.randint(draw_keys[5], (3,), 0, TOKEN_POSITIONS)
    spike_penalty = jnp.log(jax.random.uniform(draw_keys[6], (3, HEAD_NUMBER), minval=0.5, maxval=0.8))
    spike_matches = (jnp.arange(TOKEN_POSITIONS)[:, None] == spike_locations[None, :]).astype(jnp.float32)
    logarithm_decay = logarithm_decay + jnp.dot(spike_matches, spike_penalty)[:, :, None]
    return logarithm_decay.astype(jnp.bfloat16)


def block_levels(key, extent, shards, smallest, top_value):
    factor_of = 1.0
    for axis_at, parts in shards:
        draws = jax.random.uniform(jax.random.fold_in(jax.random.fold_in(key, 6), axis_at), (parts,), jnp.float32, smallest / len(shards), top_value / len(shards))
        factor_of = factor_of * jnp.repeat(jnp.exp(draws), extent[axis_at] // parts).reshape((-1,) + (1,) * (len(extent) - 1 - axis_at))
    return factor_of


def gaussian(own_key, shape, deviation, bound, cuts=(), kind=jnp.bfloat16):
    array = jax.random.normal(own_key, shape, jnp.float32) * deviation
    if len(cuts) > 0:
        array = block_levels(own_key, shape, cuts, -0.22, 0.18) * array
    return jnp.clip(array, min=-bound, max=bound).astype(kind)


def setup_inputs(seed: int = 0) -> dict:
    streams_of = jax.random.split(jax.random.key(seed), 6)
    queries = gaussian(streams_of[0], (TOKEN_POSITIONS, HEAD_NUMBER, DK), 1.0, 6.0, ((0, 8), (2, 2)))
    key_rows = gaussian(streams_of[1], (TOKEN_POSITIONS, HEAD_NUMBER, DK), 1.0, 6.0, ((0, 8), (2, 2)))
    values = gaussian(streams_of[2], (TOKEN_POSITIONS, HEAD_NUMBER, DV), 1.0, 6.0, ((0, 8), (2, 2)))
    log_decays = draw_log_decays(jax.random.fold_in(streams_of[5], 71), 0)
    output_grad = gaussian(streams_of[4], (TOKEN_POSITIONS, HEAD_NUMBER, DV), (6.0 / (DV * TOKEN_POSITIONS) ** 0.5), 0.1875, ((0, 8), (2, 2)))
    return {"queries": queries, "key_rows": key_rows, "values": values, "log_decays": log_decays, "output_grad": output_grad}


largest_entry = lax.Precision.HIGHEST


def to_blocks(tensor, length):
    row_count, head_count, channels = tensor.shape
    return tensor.astype(jnp.float32).reshape(row_count // length, length, head_count, channels).transpose(0, 2, 1, 3)


def from_blocks(tensor):
    tile_count, head_count, length, channels = tensor.shape
    return tensor.transpose(0, 2, 1, 3).reshape(tile_count * length, head_count, channels)


def causal(length):
    row_ids = lax.broadcasted_iota(jnp.int32, (length, length), 0)
    col_ids = lax.broadcasted_iota(jnp.int32, (length, length), 1)
    return row_ids >= col_ids


def reference(queries, key_rows, values, log_decays, output_grad):
    factor = DK ** -0.5
    scaled = to_blocks(queries, TILE_LEN) * factor
    keyed = to_blocks(key_rows, TILE_LEN)
    valued = to_blocks(values, TILE_LEN)
    cotangent = to_blocks(output_grad, TILE_LEN)
    cumulative = jnp.cumsum(to_blocks(log_decays, TILE_LEN), axis=2)
    lower_mask = causal(TILE_LEN)[None]
    head_count = queries.shape[1]

    def factors(local_cum):
        tile_total = local_cum[:, -1:, :]
        return jnp.exp(local_cum), jnp.exp(-local_cum), jnp.exp(tile_total - local_cum), jnp.exp(tile_total[:, 0, :])

    def forward_step(carried_over, inputs):
        query_tile, key_piece, value_piece, gradient_piece, local_cum = inputs
        growth, shrink, until_finish, piece_decay = factors(local_cum)
        scores = jnp.where(lower_mask, jnp.einsum("hiv,hjv->hij", gradient_piece, value_piece, precision=largest_entry), 0.0)
        local_part = jnp.einsum("hij,hjk->hik", scores, key_piece * shrink, precision=largest_entry)
        carried_portion = jnp.einsum("pge,pre->pgr", gradient_piece, carried_over, precision=largest_entry)
        refreshed_state = piece_decay[:, :, None] * carried_over + jnp.einsum("fnb,fne->fbe", key_piece * until_finish, value_piece, precision=largest_entry)
        return refreshed_state, growth * (local_part + carried_portion) * factor

    def backward_step(carried_over, inputs):
        query_tile, key_piece, value_piece, gradient_piece, local_cum = inputs
        growth, shrink, until_finish, piece_decay = factors(local_cum)
        amplified_query = query_tile * growth
        shrunk_key = key_piece * shrink
        attenuated_key = key_piece * until_finish
        scores = jnp.where(lower_mask, jnp.einsum("hiv,hjv->hij", gradient_piece, value_piece, precision=largest_entry), 0.0)
        key_local = shrink * jnp.einsum("hij,hik->hjk", scores, amplified_query, precision=largest_entry)
        key_passed_along = until_finish * jnp.einsum("ocb,orb->ocr", value_piece, carried_over, precision=largest_entry)
        weights = jnp.where(lower_mask, jnp.einsum("hik,hjk->hij", amplified_query, shrunk_key, precision=largest_entry), 0.0)
        value_local = jnp.einsum("hij,hiv->hjv", weights, gradient_piece, precision=largest_entry)
        value_passed_along = jnp.einsum("wbq,wqc->wbc", attenuated_key, carried_over, precision=largest_entry)
        refreshed_state = piece_decay[:, :, None] * carried_over + jnp.einsum("yaq,yao->yqo", amplified_query, gradient_piece, precision=largest_entry)
        return refreshed_state, (key_local + key_passed_along, value_local + value_passed_along)

    zero_state = jnp.zeros((head_count, DK, DV), jnp.float32)
    inputs = (scaled, keyed, valued, cotangent, cumulative)
    final_state, query_tiles = lax.scan(forward_step, zero_state, inputs)
    first_state, back_tiles = lax.scan(backward_step, zero_state, inputs, reverse=True)
    query_grad = from_blocks(query_tiles)
    key_grad = from_blocks(back_tiles[0])
    value_grad = from_blocks(back_tiles[1])
    position_grad = queries.astype(jnp.float32) * query_grad - key_rows.astype(jnp.float32) * key_grad
    decay_grad = jnp.flip(jnp.cumsum(jnp.flip(position_grad, 0), axis=0), 0)
    return query_grad, key_grad, value_grad, decay_grad
```

```python
import functools

import jax
import jax.numpy as jnp
from jax import lax
from jax.experimental import pallas as pl
from jax.experimental.pallas import tpu as pltpu
from jax.sharding import PartitionSpec as P

F32 = jnp.float32
BF16 = jnp.bfloat16
MESH = pl.DeviceIdType.MESH
LAG = 2

NN = (((1,), (0,)), ((), ()))
NT = (((1,), (1,)), ((), ()))
TN = (((0,), (0,)), ((), ()))


def mm(a, b, dims):
    return lax.dot_general(a, b, dims, preferred_element_type=F32)


def split(a):
    high = a.astype(BF16)
    return high, (a - high.astype(F32)).astype(BF16)


def kernel(
    n,
    pairs,
    factor,
    q_ref,
    k_ref,
    v_ref,
    g_ref,
    o_ref,
    dq_ref,
    dk_ref,
    dv_ref,
    dg_ref,
    qs,
    ks,
    vs,
    gs,
    os,
    grow,
    shrink,
    ends,
    decay,
    decay_in,
    own,
    peer,
    f_in,
    b_in,
    f_out,
    b_out,
    entry,
    leave,
    qk,
    qk_in,
    vg,
    vg_in,
    x_send,
    x_recv,
    f_send,
    f_recv,
    b_send,
    b_recv,
    q_send,
    q_recv,
    v_send,
    v_recv,
    d_send,
    d_recv,
):
    rows, heads, kc = q_ref.shape
    vc = v_ref.shape[2]
    half = heads // 2
    me = lax.axis_index("sa")
    ka = lax.axis_index("ka")
    vert = lax.axis_index("vert")
    pair = me // 2
    x = me % 2
    buddy = me + 1 - 2 * x
    first = pair == 0
    last = pair == pairs - 1

    barrier = pltpu.get_barrier_semaphore()

    def greet(where):
        pl.semaphore_signal(barrier, inc=1, device_id=where, device_id_type=MESH)

    greet({"sa": buddy})
    greet({"ka": 1 - ka})
    greet({"vert": 1 - vert})
    if pairs > 1:

        @pl.when(jnp.logical_not(first))
        def _():
            greet({"sa": me - 2})

        @pl.when(jnp.logical_not(last))
        def _():
            greet({"sa": me + 2})

    def remote(source, target, send, recv, where):
        return pltpu.make_async_remote_copy(
            src_ref=source,
            dst_ref=target,
            send_sem=send,
            recv_sem=recv,
            device_id=where,
            device_id_type=MESH,
        )

    def x_copy(h):
        return remote(own.at[h], peer.at[h], x_send.at[h], x_recv.at[h], {"sa": buddy})

    def d_copy():
        return remote(decay, decay_in, d_send, d_recv, {"sa": buddy})

    def f_copy(h):
        return remote(f_out.at[h], f_in.at[h], f_send.at[h], f_recv.at[h], {"sa": me + 2})

    def b_copy(h):
        return remote(b_out.at[h], b_in.at[h], b_send.at[h], b_recv.at[h], {"sa": me - 2})

    def q_copy(h, slot):
        return remote(qk.at[h], qk_in.at[slot], q_send.at[slot], q_recv.at[slot], {"vert": 1 - vert})

    def v_copy(h, slot):
        return remote(vg.at[h], vg_in.at[slot], v_send.at[slot], v_recv.at[slot], {"ka": 1 - ka})

    def stage(c, carry):
        for source, target in ((q_ref, qs), (k_ref, ks), (v_ref, vs), (g_ref, gs), (o_ref, os)):
            piece = source[pl.ds(c * 8, 8)].astype(F32)
            target[pl.ds(pl.multiple_of(c * 8 * heads, 8 * heads), 8 * heads), :] = piece.reshape(
                8 * heads, source.shape[2]
            )
        return carry

    lax.fori_loop(0, rows // 8, stage, 0)

    def head_of(s):
        return (s % 2) * half + s // 2

    def rows_of(h):
        return pl.ds(h, rows, stride=heads)

    ri = lax.broadcasted_iota(jnp.int32, (rows, rows), 0)
    ci = lax.broadcasted_iota(jnp.int32, (rows, rows), 1)
    lower = ri >= ci
    upper = ri <= ci
    tri = lower.astype(F32).astype(BF16)
    upper_ones = upper.astype(F32).astype(BF16)
    lanes = lax.broadcasted_iota(jnp.int32, (kc, 128), 1)
    token_lanes = lax.broadcasted_iota(jnp.int32, (rows, 128), 1)

    def decays(h, total):
        pick = (token_lanes == h).astype(F32).astype(BF16)
        return total + mm(gs[rows_of(h), :].astype(BF16), pick, TN)

    decay[...] = lax.fori_loop(0, heads, decays, jnp.zeros((kc, 128), F32))

    pl.semaphore_wait(
        barrier, 3 + (jnp.where(first, 0, 1) + jnp.where(last, 0, 1) if pairs > 1 else 0)
    )
    d_copy().start()

    mid = rows // 2 - 1

    def states(s, carry):
        h = head_of(s)
        g = gs[rows_of(h), :].astype(BF16)
        cum = mm(tri, g, NN)
        at_mid = cum[mid : mid + 1, :]
        at_end = cum[rows - 1 : rows, :]
        up = jnp.exp(cum - at_mid)
        down = jnp.exp(at_mid - cum)
        to_mid = jnp.exp(at_mid)
        to_end = jnp.exp(at_end - at_mid)
        grow[h] = up
        shrink[h] = down
        ends[h, 0:8, :] = jnp.broadcast_to(to_mid, (8, kc))
        ends[h, 8:16, :] = jnp.broadcast_to(to_end, (8, kc))
        key_high, key_low = split(ks[rows_of(h), :] * (down * to_end))
        query_high, query_low = split(qs[rows_of(h), :] * (up * to_mid) * factor)
        value = vs[rows_of(h), :].astype(BF16)
        cot = os[rows_of(h), :].astype(BF16)
        own[h, 0] = mm(key_high, value, TN) + mm(key_low, value, TN)
        own[h, 1] = mm(query_high, cot, TN) + mm(query_low, cot, TN)
        x_copy(h).start()
        return carry

    lax.fori_loop(0, heads, states, 0)
    d_copy().wait_recv()

    def column(ref, h):
        return jnp.exp(jnp.sum(jnp.where(lanes == h, ref[...], 0.0), axis=1, keepdims=True))

    def local(h):
        value = vs[rows_of(h), :].astype(BF16)
        cot = os[rows_of(h), :].astype(BF16)
        key_high, key_low = split(ks[rows_of(h), :] * shrink[h])
        query_high, query_low = split(qs[rows_of(h), :] * grow[h] * factor)
        s_high, s_low = split(jnp.where(lower, mm(cot, value, NT), 0.0))
        query_local = mm(s_high, key_high, NN) + mm(s_high, key_low, NN) + mm(s_low, key_high, NN)
        t_high, t_low = split(jnp.where(upper, mm(value, cot, NT), 0.0))
        key_local = (
            mm(t_high, query_high, NN) + mm(t_high, query_low, NN) + mm(t_low, query_high, NN)
        )
        qk[h, 0:rows, :] = jnp.concatenate([query_local, key_local], axis=1)
        weights = (
            mm(key_high, query_high, NT) + mm(key_high, query_low, NT) + mm(key_low, query_high, NT)
        )
        w_high, w_low = split(jnp.where(upper, weights, 0.0))
        vg[h] = mm(w_high, cot, NN) + mm(w_low, cot, NN)

    def forward(h):
        state = jnp.where(first, 0.0, f_in[h])
        e_own = column(decay, h)
        e_peer = column(decay_in, h)
        arrived = jnp.where(x == 1, peer[h, 0] + e_peer * state, state)
        entry[h] = arrived
        finish = e_own * arrived + own[h, 0]
        f_out[h] = jnp.where(x == 1, finish, e_peer * finish + peer[h, 0])

    def backward(h):
        state = jnp.where(last, 0.0, b_in[h])
        e_own = column(decay, h)
        e_peer = column(decay_in, h)
        arrived = jnp.where(x == 0, peer[h, 1] + e_peer * state, state)
        leave[h] = arrived
        start = e_own * arrived + own[h, 1]
        b_out[h] = jnp.where(x == 0, start, e_peer * start + peer[h, 1])

    def final(h):
        value = vs[rows_of(h), :].astype(BF16)
        cot = os[rows_of(h), :].astype(BF16)
        before = entry[h]
        after = leave[h]
        to_mid = ends[h, 0:1, :]
        to_end = ends[h, 8:9, :]
        i_high, i_low = split(before)
        o_high, o_low = split(after)
        query_carried = mm(cot, i_high, NT) + mm(cot, i_low, NT)
        key_carried = mm(value, o_high, NT) + mm(value, o_low, NT)
        both = qk[h, 0:rows, :]
        up = grow[h]
        down = shrink[h]
        query_part = up * (both[:, :kc] + to_mid * query_carried) * factor
        key_part = down * (both[:, kc:] + to_end * key_carried)
        qk[h, 0:rows, :] = jnp.concatenate([query_part, key_part], axis=1)
        key_high, key_low = split(ks[rows_of(h), :] * (down * to_end))
        vg[h] = vg[h] + (
            mm(key_high, o_high, NN) + mm(key_high, o_low, NN) + mm(key_low, o_high, NN)
        )
        crossing = (column(decay, h) * before + own[h, 0]) * after
        c_high, c_low = split(crossing)
        ones = jnp.ones((8, vc), BF16)
        beyond = mm(ones, c_high, NT) + mm(ones, c_low, NT)
        qk[h, rows : rows + 8, :] = jnp.concatenate([beyond, beyond], axis=1)

    wait_end = LAG * (pairs - 1)
    f_lag = LAG * pair
    b_lag = LAG * (pairs - 1 - pair)
    c_lag = jnp.maximum(f_lag, b_lag)

    def step(s, carry):
        @pl.when(s < heads)
        def _():
            h = head_of(s)
            local(h)
            x_copy(h).wait_recv()

        fs = s - f_lag

        @pl.when(jnp.logical_and(fs >= 0, fs < heads))
        def _():
            h = head_of(fs)
            if pairs > 1:

                @pl.when(jnp.logical_not(first))
                def _():
                    f_copy(h).wait_recv()

            forward(h)
            if pairs > 1:

                @pl.when(jnp.logical_not(last))
                def _():
                    f_copy(h).start()

        bs = s - b_lag

        @pl.when(jnp.logical_and(bs >= 0, bs < heads))
        def _():
            h = head_of(bs)
            if pairs > 1:

                @pl.when(jnp.logical_not(last))
                def _():
                    b_copy(h).wait_recv()

            backward(h)
            if pairs > 1:

                @pl.when(jnp.logical_not(first))
                def _():
                    b_copy(h).start()

        cs = s - c_lag

        @pl.when(jnp.logical_and(cs >= 0, cs < heads))
        def _():
            h = head_of(cs)
            final(h)
            slot = h % half

            @pl.when(h // half != vert)
            def _():
                q_copy(h, slot).start()

            @pl.when(h // half != ka)
            def _():
                v_copy(h, slot).start()

        return carry

    lax.fori_loop(0, heads + wait_end, step, 0)

    def combine(i, carry):
        h = vert * half + i
        q_copy(h, i).wait_recv()
        total = qk[h] + qk_in[i]
        query_grad = total[0:rows, :kc]
        key_grad = total[0:rows, kc:]
        dq_ref[pl.ds(i, rows, stride=half), :] = query_grad
        dk_ref[pl.ds(i, rows, stride=half), :] = key_grad
        position = qs[rows_of(h), :] * query_grad - ks[rows_of(h), :] * key_grad
        p_high, p_low = split(position)
        sums = mm(upper_ones, p_high, NN) + mm(upper_ones, p_low, NN)
        dg_ref[pl.ds(i, rows, stride=half), :] = sums + total[rows : rows + 1, :kc]
        hv = ka * half + i
        v_copy(hv, i).wait_recv()
        dv_ref[pl.ds(i, rows, stride=half), :] = vg[hv] + vg_in[i]
        return carry

    lax.fori_loop(0, half, combine, 0)

    d_copy().wait_send()

    def drain(h, carry):
        x_copy(h).wait_send()
        if pairs > 1:

            @pl.when(jnp.logical_not(last))
            def _():
                f_copy(h).wait_send()

            @pl.when(jnp.logical_not(first))
            def _():
                b_copy(h).wait_send()

        return carry

    lax.fori_loop(0, heads, drain, 0)

    def drain_parts(i, carry):
        q_copy((1 - vert) * half + i, i).wait_send()
        v_copy((1 - ka) * half + i, i).wait_send()
        return carry

    lax.fori_loop(0, half, drain_parts, 0)


def shards(queries, key_rows, values, log_decays, output_grad):
    rows, heads, kc = queries.shape
    vc = values.shape[2]
    n = lax.axis_size("sa")
    half = heads // 2
    factor = (kc * lax.axis_size("ka")) ** -0.5
    dma = pltpu.SemaphoreType.DMA
    vmem = pl.BlockSpec(memory_space=pltpu.VMEM)
    narrow = jax.ShapeDtypeStruct((rows * half, kc), F32)
    wide = jax.ShapeDtypeStruct((rows * half, vc), F32)
    outs = pl.pallas_call(
        functools.partial(kernel, n, n // 2, factor),
        out_shape=(narrow, narrow, wide, narrow),
        in_specs=[vmem] * 5,
        out_specs=(vmem,) * 4,
        scratch_shapes=[
            pltpu.VMEM((rows * heads, kc), F32),
            pltpu.VMEM((rows * heads, kc), F32),
            pltpu.VMEM((rows * heads, vc), F32),
            pltpu.VMEM((rows * heads, kc), F32),
            pltpu.VMEM((rows * heads, vc), F32),
            pltpu.VMEM((heads, rows, kc), F32),
            pltpu.VMEM((heads, rows, kc), F32),
            pltpu.VMEM((heads, 16, kc), F32),
            pltpu.VMEM((kc, 128), F32),
            pltpu.VMEM((kc, 128), F32),
            pltpu.VMEM((heads, 2, kc, vc), F32),
            pltpu.VMEM((heads, 2, kc, vc), F32),
            pltpu.VMEM((heads, kc, vc), F32),
            pltpu.VMEM((heads, kc, vc), F32),
            pltpu.VMEM((heads, kc, vc), F32),
            pltpu.VMEM((heads, kc, vc), F32),
            pltpu.VMEM((heads, kc, vc), F32),
            pltpu.VMEM((heads, kc, vc), F32),
            pltpu.VMEM((heads, rows + 8, 2 * kc), F32),
            pltpu.VMEM((half, rows + 8, 2 * kc), F32),
            pltpu.VMEM((heads, rows, vc), F32),
            pltpu.VMEM((half, rows, vc), F32),
            dma((heads,)),
            dma((heads,)),
            dma((heads,)),
            dma((heads,)),
            dma((heads,)),
            dma((heads,)),
            dma((half,)),
            dma((half,)),
            dma((half,)),
            dma((half,)),
            dma,
            dma,
        ],
        compiler_params=pltpu.CompilerParams(
            collective_id=0, has_side_effects=True, vmem_limit_bytes=48 * 1024 * 1024
        ),
    )(queries, key_rows, values, log_decays, output_grad)
    query_grad, key_grad, value_grad, decay_grad = outs
    return (
        query_grad.reshape(rows, half, kc),
        key_grad.reshape(rows, half, kc),
        value_grad.reshape(rows, half, vc),
        decay_grad.reshape(rows, half, kc),
    )


def solution(mesh):
    return jax.shard_map(
        shards,
        mesh=mesh,
        in_specs=(
            P("sa", None, "ka"),
            P("sa", None, "ka"),
            P("sa", None, "vert"),
            P("sa", None, "ka"),
            P("sa", None, "vert"),
        ),
        out_specs=(
            P("sa", "vert", "ka"),
            P("sa", "vert", "ka"),
            P("sa", "ka", "vert"),
            P("sa", "vert", "ka"),
        ),
        check_vma=False,
    )
```

```python
import functools

import jax
import jax.numpy as jnp
from jax import lax
from jax.experimental import pallas as pl
from jax.experimental.pallas import tpu as pltpu
from jax.sharding import PartitionSpec as P

F32 = jnp.float32
BF16 = jnp.bfloat16
MESH = pl.DeviceIdType.MESH
LAG = 2

NN = (((1,), (0,)), ((), ()))
NT = (((1,), (1,)), ((), ()))
TN = (((0,), (0,)), ((), ()))


def mm(a, b, dims):
    return lax.dot_general(a, b, dims, preferred_element_type=F32)


def split(a):
    high = a.astype(BF16)
    return high, (a - high.astype(F32)).astype(BF16)


def kernel(
    n,
    pairs,
    factor,
    q_ref,
    k_ref,
    v_ref,
    g_ref,
    o_ref,
    dq_ref,
    dk_ref,
    dv_ref,
    dg_ref,
    vs,
    os,
    grow,
    shrink,
    ends,
    decay,
    decay_in,
    own,
    peer,
    f_in,
    b_in,
    f_out,
    b_out,
    entry,
    leave,
    qk,
    qk_in,
    vg,
    vg_in,
    x_send,
    x_recv,
    f_send,
    f_recv,
    b_send,
    b_recv,
    q_send,
    q_recv,
    v_send,
    v_recv,
    d_send,
    d_recv,
):
    heads, kc, rows = q_ref.shape
    vc = v_ref.shape[2]
    half = heads // 2
    me = lax.axis_index("sa")
    ka = lax.axis_index("ka")
    vert = lax.axis_index("vert")
    pair = me // 2
    x = me % 2
    buddy = me + 1 - 2 * x
    first = pair == 0
    last = pair == pairs - 1

    barrier = pltpu.get_barrier_semaphore()

    def greet(where):
        pl.semaphore_signal(barrier, inc=1, device_id=where, device_id_type=MESH)

    greet({"sa": buddy})
    greet({"ka": 1 - ka})
    greet({"vert": 1 - vert})
    if pairs > 1:

        @pl.when(jnp.logical_not(first))
        def _():
            greet({"sa": me - 2})

        @pl.when(jnp.logical_not(last))
        def _():
            greet({"sa": me + 2})

    def remote(source, target, send, recv, where):
        return pltpu.make_async_remote_copy(
            src_ref=source,
            dst_ref=target,
            send_sem=send,
            recv_sem=recv,
            device_id=where,
            device_id_type=MESH,
        )

    def x_copy(h):
        return remote(own.at[h], peer.at[h], x_send.at[h], x_recv.at[h], {"sa": buddy})

    def d_copy():
        return remote(decay, decay_in, d_send, d_recv, {"sa": buddy})

    def f_copy(h):
        return remote(f_out.at[h], f_in.at[h], f_send.at[h], f_recv.at[h], {"sa": me + 2})

    def b_copy(h):
        return remote(b_out.at[h], b_in.at[h], b_send.at[h], b_recv.at[h], {"sa": me - 2})

    def q_copy(h, slot):
        return remote(qk.at[h], qk_in.at[slot], q_send.at[slot], q_recv.at[slot], {"vert": 1 - vert})

    def v_copy(h, slot):
        return remote(vg.at[h], vg_in.at[slot], v_send.at[slot], v_recv.at[slot], {"ka": 1 - ka})

    def stage(c, carry):
        for source, target in ((v_ref, vs), (o_ref, os)):
            piece = source[pl.ds(c * 8, 8)].astype(F32)
            target[pl.ds(pl.multiple_of(c * 8 * heads, 8 * heads), 8 * heads), :] = piece.reshape(
                8 * heads, source.shape[2]
            )
        return carry

    lax.fori_loop(0, rows // 8, stage, 0)

    def head_of(s):
        return (s % 2) * half + s // 2

    def rows_of(h):
        return pl.ds(h, rows, stride=heads)

    ri = lax.broadcasted_iota(jnp.int32, (rows, rows), 0)
    ci = lax.broadcasted_iota(jnp.int32, (rows, rows), 1)
    lower = ri >= ci
    upper = ri <= ci
    upper_ones = upper.astype(F32).astype(BF16)
    lower_ones = lower.astype(F32).astype(BF16)
    lanes = lax.broadcasted_iota(jnp.int32, (kc, 128), 1)

    def decays(h, total):
        pick = (ci == h).astype(F32).astype(BF16)
        return total + mm(g_ref[h], pick, NN)

    decay[...] = lax.fori_loop(0, heads, decays, jnp.zeros((kc, 128), F32))

    pl.semaphore_wait(
        barrier, 3 + (jnp.where(first, 0, 1) + jnp.where(last, 0, 1) if pairs > 1 else 0)
    )
    d_copy().start()

    mid = rows // 2 - 1

    def states(s, carry):
        h = head_of(s)
        cum = mm(g_ref[h], upper_ones, NN)
        at_mid = cum[:, mid : mid + 1]
        at_end = cum[:, rows - 1 : rows]
        up = jnp.exp(cum - at_mid)
        down = jnp.exp(at_mid - cum)
        to_mid = jnp.exp(at_mid)
        to_end = jnp.exp(at_end - at_mid)
        grow[h] = up
        shrink[h] = down
        ends[h, 0] = jnp.broadcast_to(to_mid, (kc, rows))
        ends[h, 1] = jnp.broadcast_to(to_end, (kc, rows))
        key_high, key_low = split(k_ref[h].astype(F32) * (down * to_end))
        query_high, query_low = split(q_ref[h].astype(F32) * (up * to_mid) * factor)
        value = vs[rows_of(h), :].astype(BF16)
        cot = os[rows_of(h), :].astype(BF16)
        own[h, 0] = mm(key_high, value, NN) + mm(key_low, value, NN)
        own[h, 1] = mm(query_high, cot, NN) + mm(query_low, cot, NN)
        x_copy(h).start()
        return carry

    lax.fori_loop(0, heads, states, 0)
    d_copy().wait_recv()

    def column(ref, h):
        return jnp.exp(jnp.sum(jnp.where(lanes == h, ref[...], 0.0), axis=1, keepdims=True))

    def local(h):
        value = vs[rows_of(h), :].astype(BF16)
        cot = os[rows_of(h), :].astype(BF16)
        key_high, key_low = split(k_ref[h].astype(F32) * shrink[h])
        query_high, query_low = split(q_ref[h].astype(F32) * grow[h] * factor)
        t_high, t_low = split(jnp.where(upper, mm(value, cot, NT), 0.0))
        qk[h, 0:kc] = mm(key_high, t_high, NN) + mm(key_low, t_high, NN) + mm(key_high, t_low, NN)
        s_high, s_low = split(jnp.where(lower, mm(cot, value, NT), 0.0))
        qk[h, kc : 2 * kc] = (
            mm(query_high, s_high, NN) + mm(query_low, s_high, NN) + mm(query_high, s_low, NN)
        )
        weights = (
            mm(key_high, query_high, TN) + mm(key_high, query_low, TN) + mm(key_low, query_high, TN)
        )
        w_high, w_low = split(jnp.where(upper, weights, 0.0))
        vg[h] = mm(w_high, cot, NN) + mm(w_low, cot, NN)

    def forward(h):
        state = jnp.where(first, 0.0, f_in[h])
        e_own = column(decay, h)
        e_peer = column(decay_in, h)
        arrived = jnp.where(x == 1, peer[h, 0] + e_peer * state, state)
        entry[h] = arrived
        finish = e_own * arrived + own[h, 0]
        f_out[h] = jnp.where(x == 1, finish, e_peer * finish + peer[h, 0])

    def backward(h):
        state = jnp.where(last, 0.0, b_in[h])
        e_own = column(decay, h)
        e_peer = column(decay_in, h)
        arrived = jnp.where(x == 0, peer[h, 1] + e_peer * state, state)
        leave[h] = arrived
        start = e_own * arrived + own[h, 1]
        b_out[h] = jnp.where(x == 0, start, e_peer * start + peer[h, 1])

    def final(h):
        value = vs[rows_of(h), :].astype(BF16)
        cot = os[rows_of(h), :].astype(BF16)
        before = entry[h]
        after = leave[h]
        to_mid = ends[h, 0]
        to_end = ends[h, 1]
        i_high, i_low = split(before)
        o_high, o_low = split(after)
        query_carried = mm(i_high, cot, NT) + mm(i_low, cot, NT)
        key_carried = mm(o_high, value, NT) + mm(o_low, value, NT)
        down = shrink[h]
        qk[h, 0:kc] = grow[h] * (qk[h, 0:kc] + to_mid * query_carried) * factor
        qk[h, kc : 2 * kc] = down * (qk[h, kc : 2 * kc] + to_end * key_carried)
        key_high, key_low = split(k_ref[h].astype(F32) * (down * to_end))
        vg[h] = vg[h] + (
            mm(key_high, o_high, TN) + mm(key_high, o_low, TN) + mm(key_low, o_high, TN)
        )
        crossing = (column(decay, h) * before + own[h, 0]) * after
        beyond = jnp.sum(crossing, axis=1, keepdims=True)
        qk[h, 2 * kc : 3 * kc] = jnp.broadcast_to(beyond, (kc, rows))

    wait_end = LAG * (pairs - 1)
    f_lag = LAG * pair
    b_lag = LAG * (pairs - 1 - pair)
    c_lag = jnp.maximum(f_lag, b_lag)

    def step(s, carry):
        @pl.when(s < heads)
        def _():
            h = head_of(s)
            local(h)
            x_copy(h).wait_recv()

        fs = s - f_lag

        @pl.when(jnp.logical_and(fs >= 0, fs < heads))
        def _():
            h = head_of(fs)
            if pairs > 1:

                @pl.when(jnp.logical_not(first))
                def _():
                    f_copy(h).wait_recv()

            forward(h)
            if pairs > 1:

                @pl.when(jnp.logical_not(last))
                def _():
                    f_copy(h).start()

        bs = s - b_lag

        @pl.when(jnp.logical_and(bs >= 0, bs < heads))
        def _():
            h = head_of(bs)
            if pairs > 1:

                @pl.when(jnp.logical_not(last))
                def _():
                    b_copy(h).wait_recv()

            backward(h)
            if pairs > 1:

                @pl.when(jnp.logical_not(first))
                def _():
                    b_copy(h).start()

        cs = s - c_lag

        @pl.when(jnp.logical_and(cs >= 0, cs < heads))
        def _():
            h = head_of(cs)
            final(h)
            slot = h % half

            @pl.when(h // half != vert)
            def _():
                q_copy(h, slot).start()

            @pl.when(h // half != ka)
            def _():
                v_copy(h, slot).start()

        return carry

    lax.fori_loop(0, heads + wait_end, step, 0)

    def combine(i, carry):
        h = vert * half + i
        q_copy(h, i).wait_recv()
        query_grad = qk[h, 0:kc] + qk_in[i, 0:kc]
        key_grad = qk[h, kc : 2 * kc] + qk_in[i, kc : 2 * kc]
        dq_ref[i] = query_grad
        dk_ref[i] = key_grad
        position = q_ref[h].astype(F32) * query_grad - k_ref[h].astype(F32) * key_grad
        p_high, p_low = split(position)
        sums = mm(p_high, lower_ones, NN) + mm(p_low, lower_ones, NN)
        dg_ref[i] = sums + (qk[h, 2 * kc : 3 * kc] + qk_in[i, 2 * kc : 3 * kc])
        hv = ka * half + i
        v_copy(hv, i).wait_recv()
        dv_ref[pl.ds(i, rows, stride=half), :] = vg[hv] + vg_in[i]
        return carry

    lax.fori_loop(0, half, combine, 0)

    d_copy().wait_send()

    def drain(h, carry):
        x_copy(h).wait_send()
        if pairs > 1:

            @pl.when(jnp.logical_not(last))
            def _():
                f_copy(h).wait_send()

            @pl.when(jnp.logical_not(first))
            def _():
                b_copy(h).wait_send()

        return carry

    lax.fori_loop(0, heads, drain, 0)

    def drain_parts(i, carry):
        q_copy((1 - vert) * half + i, i).wait_send()
        v_copy((1 - ka) * half + i, i).wait_send()
        return carry

    lax.fori_loop(0, half, drain_parts, 0)


def shards(queries, key_rows, values, log_decays, output_grad):
    rows, heads, kc = queries.shape
    vc = values.shape[2]
    n = lax.axis_size("sa")
    half = heads // 2
    factor = (kc * lax.axis_size("ka")) ** -0.5
    dma = pltpu.SemaphoreType.DMA
    vmem = pl.BlockSpec(memory_space=pltpu.VMEM)
    narrow = jax.ShapeDtypeStruct((half, kc, rows), F32)
    wide = jax.ShapeDtypeStruct((rows * half, vc), F32)
    outs = pl.pallas_call(
        functools.partial(kernel, n, n // 2, factor),
        out_shape=(narrow, narrow, wide, narrow),
        in_specs=[vmem] * 5,
        out_specs=(vmem,) * 4,
        scratch_shapes=[
            pltpu.VMEM((rows * heads, vc), F32),
            pltpu.VMEM((rows * heads, vc), F32),
            pltpu.VMEM((heads, kc, rows), F32),
            pltpu.VMEM((heads, kc, rows), F32),
            pltpu.VMEM((heads, 2, kc, rows), F32),
            pltpu.VMEM((kc, 128), F32),
            pltpu.VMEM((kc, 128), F32),
            pltpu.VMEM((heads, 2, kc, vc), F32),
            pltpu.VMEM((heads, 2, kc, vc), F32),
            pltpu.VMEM((heads, kc, vc), F32),
            pltpu.VMEM((heads, kc, vc), F32),
            pltpu.VMEM((heads, kc, vc), F32),
            pltpu.VMEM((heads, kc, vc), F32),
            pltpu.VMEM((heads, kc, vc), F32),
            pltpu.VMEM((heads, kc, vc), F32),
            pltpu.VMEM((heads, 3 * kc, rows), F32),
            pltpu.VMEM((half, 3 * kc, rows), F32),
            pltpu.VMEM((heads, rows, vc), F32),
            pltpu.VMEM((half, rows, vc), F32),
            dma((heads,)),
            dma((heads,)),
            dma((heads,)),
            dma((heads,)),
            dma((heads,)),
            dma((heads,)),
            dma((half,)),
            dma((half,)),
            dma((half,)),
            dma((half,)),
            dma,
            dma,
        ],
        compiler_params=pltpu.CompilerParams(
            collective_id=0, has_side_effects=True, vmem_limit_bytes=48 * 1024 * 1024
        ),
    )(
        queries.transpose(1, 2, 0),
        key_rows.transpose(1, 2, 0),
        values,
        log_decays.transpose(1, 2, 0),
        output_grad,
    )
    query_grad, key_grad, value_grad, decay_grad = outs
    return (
        query_grad.transpose(2, 0, 1),
        key_grad.transpose(2, 0, 1),
        value_grad.reshape(rows, half, vc),
        decay_grad.transpose(2, 0, 1),
    )


def solution(mesh):
    return jax.shard_map(
        shards,
        mesh=mesh,
        in_specs=(
            P("sa", None, "ka"),
            P("sa", None, "ka"),
            P("sa", None, "vert"),
            P("sa", None, "ka"),
            P("sa", None, "vert"),
        ),
        out_specs=(
            P("sa", "vert", "ka"),
            P("sa", "vert", "ka"),
            P("sa", "ka", "vert"),
            P("sa", "vert", "ka"),
        ),
        check_vma=False,
    )
```

```python
import functools

import jax
import jax.numpy as jnp
from jax import lax
from jax.experimental import pallas as pl
from jax.experimental.pallas import tpu as pltpu
from jax.sharding import PartitionSpec as P

F32 = jnp.float32
BF16 = jnp.bfloat16
MESH = pl.DeviceIdType.MESH
LAG = 2

NN = (((1,), (0,)), ((), ()))
NT = (((1,), (1,)), ((), ()))
TN = (((0,), (0,)), ((), ()))


def mm(a, b, dims):
    return lax.dot_general(a, b, dims, preferred_element_type=F32)


def split(a):
    high = a.astype(BF16)
    return high, (a - high.astype(F32)).astype(BF16)


def kernel(
    n,
    pairs,
    factor,
    q_hbm,
    k_hbm,
    v_hbm,
    g_hbm,
    o_hbm,
    dq_ref,
    dk_ref,
    dv_ref,
    dg_ref,
    q_ref,
    k_ref,
    v_ref,
    g_ref,
    o_ref,
    vs,
    os,
    vb,
    ob,
    e_own,
    e_peer,
    grow,
    shrink,
    ends,
    decay,
    decay_in,
    own,
    peer,
    f_in,
    b_in,
    f_out,
    b_out,
    x_out,
    entry,
    leave,
    qk,
    qk_in,
    vg,
    vg_in,
    x_send,
    x_recv,
    f_send,
    f_recv,
    b_send,
    b_recv,
    q_send,
    q_recv,
    v_send,
    v_recv,
    d_send,
    d_recv,
    y_send,
    y_recv,
    w_send,
    w_recv,
    in_sem,
):
    heads, kc, rows = q_ref.shape
    vc = v_ref.shape[2]
    half = heads // 2
    quarter = half // 2
    loads = [
        pltpu.make_async_copy(source, target, in_sem.at[i])
        for i, (source, target) in enumerate(
            ((g_hbm, g_ref), (v_hbm, v_ref), (o_hbm, o_ref), (k_hbm, k_ref), (q_hbm, q_ref))
        )
    ]
    for load in loads:
        load.start()
    me = lax.axis_index("sa")
    ka = lax.axis_index("ka")
    vert = lax.axis_index("vert")
    pair = me // 2
    x = me % 2
    buddy = me + 1 - 2 * x
    first = pair == 0
    last = pair == pairs - 1

    barrier = pltpu.get_barrier_semaphore()

    def greet(where):
        pl.semaphore_signal(barrier, inc=1, device_id=where, device_id_type=MESH)

    greet({"sa": buddy})
    greet({"ka": 1 - ka})
    greet({"vert": 1 - vert})
    if pairs > 1:

        @pl.when(jnp.logical_not(first))
        def _():
            greet({"sa": me - 2})

        @pl.when(jnp.logical_not(last))
        def _():
            greet({"sa": me + 2})

    def remote(source, target, send, recv, where):
        return pltpu.make_async_remote_copy(
            src_ref=source,
            dst_ref=target,
            send_sem=send,
            recv_sem=recv,
            device_id=where,
            device_id_type=MESH,
        )

    def x_copy(h):
        return remote(own.at[h], peer.at[h], x_send.at[h], x_recv.at[h], {"sa": buddy})

    def y_copy(h):
        return remote(
            x_out.at[h, 0], peer.at[h, 0], y_send.at[h], y_recv.at[h], {"sa": buddy}
        )

    def w_copy(h):
        return remote(
            x_out.at[h, 1], peer.at[h, 1], w_send.at[h], w_recv.at[h], {"sa": buddy}
        )

    def d_copy():
        return remote(decay, decay_in, d_send, d_recv, {"sa": buddy})

    def f_copy(h):
        return remote(f_out.at[h], f_in.at[h], f_send.at[h], f_recv.at[h], {"sa": me + 2})

    def b_copy(h):
        return remote(b_out.at[h], b_in.at[h], b_send.at[h], b_recv.at[h], {"sa": me - 2})

    def q_copy(h, slot):
        return remote(qk.at[h], qk_in.at[slot], q_send.at[slot], q_recv.at[slot], {"vert": 1 - vert})

    def v_copy(h, slot):
        return remote(vg.at[h], vg_in.at[slot], v_send.at[slot], v_recv.at[slot], {"ka": 1 - ka})

    def first_set(j):
        return (j % 2) * half + j // 2

    def second_set(j):
        return first_set(j) + quarter

    def rows_of(h):
        return pl.ds(h, rows, stride=heads)

    ri = lax.broadcasted_iota(jnp.int32, (rows, rows), 0)
    ci = lax.broadcasted_iota(jnp.int32, (rows, rows), 1)
    lower = ri >= ci
    upper = ri <= ci
    upper_ones = upper.astype(F32).astype(BF16)
    lower_ones = lower.astype(F32).astype(BF16)
    lanes = lax.broadcasted_iota(jnp.int32, (kc, 128), 1)

    loads[0].wait()
    ones = jnp.ones((rows, 128), BF16)
    packed = jnp.zeros((kc, 128), F32)
    for h in range(heads):
        total = mm(g_ref[h], ones, NN)
        e_own[h] = jnp.exp(total)
        packed = jnp.where(lanes == h, total, packed)
    decay[...] = packed

    pl.semaphore_wait(
        barrier, 3 + (jnp.where(first, 0, 1) + jnp.where(last, 0, 1) if pairs > 1 else 0)
    )
    d_copy().start()

    for load in loads[1:]:
        load.wait()

    def stage(c, carry):
        for source, target in ((v_ref, vs), (o_ref, os)):
            piece = source[pl.ds(c * 8, 8)].astype(F32)
            target[pl.ds(pl.multiple_of(c * 8 * heads, 8 * heads), 8 * heads), :] = piece.reshape(
                8 * heads, source.shape[2]
            )
        return carry

    lax.fori_loop(0, rows // 8, stage, 0, unroll=4)

    mid = rows // 2 - 1

    def states(h):
        cum = mm(g_ref[h], upper_ones, NN)
        at_mid = cum[:, mid : mid + 1]
        at_end = cum[:, rows - 1 : rows]
        up = jnp.exp(cum - at_mid)
        down = jnp.exp(at_mid - cum)
        to_mid = jnp.exp(at_mid)
        to_end = jnp.exp(at_end - at_mid)
        grow[h] = up
        shrink[h] = down
        ends[h, 0] = jnp.broadcast_to(to_mid, (kc, rows))
        ends[h, 1] = jnp.broadcast_to(to_end, (kc, rows))
        key_high, key_low = split(k_ref[h].astype(F32) * (down * to_end))
        query_high, query_low = split(q_ref[h].astype(F32) * (up * to_mid) * factor)
        value = vs[rows_of(h), :].astype(BF16)
        cot = os[rows_of(h), :].astype(BF16)
        vb[h] = value
        ob[h] = cot
        own[h, 0] = mm(key_high, value, NN) + mm(key_low, value, NN)
        own[h, 1] = mm(query_high, cot, NN) + mm(query_low, cot, NN)

    def early(i, carry):
        for j in (2 * i, 2 * i + 1):
            states(first_set(j))
        for j in (2 * i, 2 * i + 1):
            x_copy(first_set(j)).start()
        return carry

    lax.fori_loop(0, quarter, early, 0)
    d_copy().wait_recv()
    received = decay_in[...]
    for h in range(heads):
        e_peer[h] = jnp.exp(jnp.broadcast_to(received[:, h : h + 1], (kc, 128)))

    def local(h):
        value = vb[h]
        cot = ob[h]
        key_high, key_low = split(k_ref[h].astype(F32) * shrink[h])
        query_high, query_low = split(q_ref[h].astype(F32) * grow[h] * factor)
        t_high, t_low = split(jnp.where(upper, mm(value, cot, NT), 0.0))
        qk[h, 0:kc] = mm(key_high, t_high, NN) + mm(key_low, t_high, NN) + mm(key_high, t_low, NN)
        s_high, s_low = split(jnp.where(lower, mm(cot, value, NT), 0.0))
        qk[h, kc : 2 * kc] = (
            mm(query_high, s_high, NN) + mm(query_low, s_high, NN) + mm(query_high, s_low, NN)
        )
        weights = (
            mm(key_high, query_high, TN) + mm(key_high, query_low, TN) + mm(key_low, query_high, TN)
        )
        w_high, w_low = split(jnp.where(upper, weights, 0.0))
        vg[h] = mm(w_high, cot, NN) + mm(w_low, cot, NN)

    def forward_pair(h):
        state = jnp.where(first, 0.0, f_in[h])
        arrived = jnp.where(x == 1, peer[h, 0] + e_peer[h] * state, state)
        entry[h] = arrived
        finish = e_own[h] * arrived + own[h, 0]
        f_out[h] = jnp.where(x == 1, finish, e_peer[h] * finish + peer[h, 0])

    def backward_pair(h):
        state = jnp.where(last, 0.0, b_in[h])
        arrived = jnp.where(x == 0, peer[h, 1] + e_peer[h] * state, state)
        leave[h] = arrived
        start = e_own[h] * arrived + own[h, 1]
        b_out[h] = jnp.where(x == 0, start, e_peer[h] * start + peer[h, 1])

    def forward_column(h):
        state = jnp.where(first, 0.0, f_in[h])
        finish = e_own[h] * state + own[h, 0]
        across = e_peer[h] * state
        entry[h] = jnp.where(x == 0, state, across)
        x_out[h, 0] = jnp.where(x == 0, finish, state)
        f_out[h] = jnp.where(x == 0, e_peer[h] * finish, e_own[h] * across + own[h, 0])

    def backward_column(h):
        state = jnp.where(last, 0.0, b_in[h])
        start = e_own[h] * state + own[h, 1]
        across = e_peer[h] * state
        leave[h] = jnp.where(x == 1, state, across)
        x_out[h, 1] = jnp.where(x == 1, start, state)
        b_out[h] = jnp.where(x == 1, e_peer[h] * start, e_own[h] * across + own[h, 1])

    def final(h, before, after):
        value = vb[h]
        cot = ob[h]
        to_mid = ends[h, 0]
        to_end = ends[h, 1]
        i_high, i_low = split(before)
        o_high, o_low = split(after)
        query_carried = mm(i_high, cot, NT) + mm(i_low, cot, NT)
        key_carried = mm(o_high, value, NT) + mm(o_low, value, NT)
        down = shrink[h]
        qk[h, 0:kc] = grow[h] * (qk[h, 0:kc] + to_mid * query_carried) * factor
        qk[h, kc : 2 * kc] = down * (qk[h, kc : 2 * kc] + to_end * key_carried)
        key_high, key_low = split(k_ref[h].astype(F32) * (down * to_end))
        vg[h] = vg[h] + (
            mm(key_high, o_high, TN) + mm(key_high, o_low, TN) + mm(key_low, o_high, TN)
        )
        crossing = (e_own[h] * before + own[h, 0]) * after
        beyond = jnp.sum(crossing, axis=1, keepdims=True)
        qk[h, 2 * kc : 3 * kc] = jnp.broadcast_to(beyond, (kc, rows))

    f_lag = LAG * pair
    b_lag = LAG * (pairs - 1 - pair)
    c_lag = jnp.maximum(f_lag, b_lag)
    second_lag = max(half, LAG * (pairs - 1) + 2)

    def forward_in(h):
        if pairs > 1:

            @pl.when(jnp.logical_not(first))
            def _():
                f_copy(h).wait_recv()

    def forward_on(h):
        if pairs > 1:

            @pl.when(jnp.logical_not(last))
            def _():
                f_copy(h).start()

    def backward_in(h):
        if pairs > 1:

            @pl.when(jnp.logical_not(last))
            def _():
                b_copy(h).wait_recv()

    def backward_on(h):
        if pairs > 1:

            @pl.when(jnp.logical_not(first))
            def _():
                b_copy(h).start()

    def send_parts(h):
        slot = h % half

        @pl.when(h // half != vert)
        def _():
            q_copy(h, slot).start()

        @pl.when(h // half != ka)
        def _():
            v_copy(h, slot).start()

    def inside(j):
        return jnp.logical_and(j >= 0, j < half)

    def step(t, carry):
        @pl.when(t < half)
        def _():
            states(second_set(t))
            local(first_set(t))
            x_copy(first_set(t)).wait_recv()

        @pl.when(inside(t - half))
        def _():
            local(second_set(t - half))

        fj = t - f_lag

        @pl.when(inside(fj))
        def _():
            column = second_set(fj)
            forward_in(column)
            forward_column(column)
            forward_on(column)
            y_copy(column).start()
            paired = first_set(fj)
            forward_in(paired)
            forward_pair(paired)
            forward_on(paired)

        bj = t - b_lag

        @pl.when(inside(bj))
        def _():
            column = second_set(bj)
            backward_in(column)
            backward_column(column)
            backward_on(column)
            w_copy(column).start()
            paired = first_set(bj)
            backward_in(paired)
            backward_pair(paired)
            backward_on(paired)

        cj = t - c_lag

        @pl.when(inside(cj))
        def _():
            h = first_set(cj)
            final(h, entry[h], leave[h])
            send_parts(h)

        sj = t - second_lag

        @pl.when(inside(sj))
        def _():
            h = second_set(sj)
            y_copy(h).wait_recv()
            w_copy(h).wait_recv()
            final(h, entry[h] + peer[h, 0], leave[h] + peer[h, 1])
            send_parts(h)

        return carry

    lax.fori_loop(0, half + second_lag, step, 0)

    def combine(i, carry):
        h = vert * half + i
        q_copy(h, i).wait_recv()
        query_grad = qk[h, 0:kc] + qk_in[i, 0:kc]
        key_grad = qk[h, kc : 2 * kc] + qk_in[i, kc : 2 * kc]
        dq_ref[i] = query_grad
        dk_ref[i] = key_grad
        position = q_ref[h].astype(F32) * query_grad - k_ref[h].astype(F32) * key_grad
        p_high, p_low = split(position)
        sums = mm(p_high, lower_ones, NN) + mm(p_low, lower_ones, NN)
        dg_ref[i] = sums + (qk[h, 2 * kc : 3 * kc] + qk_in[i, 2 * kc : 3 * kc])
        hv = ka * half + i
        v_copy(hv, i).wait_recv()
        dv_ref[pl.ds(i, rows, stride=half), :] = vg[hv] + vg_in[i]
        return carry

    lax.fori_loop(0, half, combine, 0)

    d_copy().wait_send()

    def drain(h, carry):
        if pairs > 1:

            @pl.when(jnp.logical_not(last))
            def _():
                f_copy(h).wait_send()

            @pl.when(jnp.logical_not(first))
            def _():
                b_copy(h).wait_send()

        return carry

    lax.fori_loop(0, heads, drain, 0)

    def drain_x(j, carry):
        x_copy(first_set(j)).wait_send()
        y_copy(second_set(j)).wait_send()
        w_copy(second_set(j)).wait_send()
        return carry

    lax.fori_loop(0, half, drain_x, 0)

    def drain_parts(i, carry):
        q_copy((1 - vert) * half + i, i).wait_send()
        v_copy((1 - ka) * half + i, i).wait_send()
        return carry

    lax.fori_loop(0, half, drain_parts, 0)


def shards(queries, key_rows, values, log_decays, output_grad):
    rows, heads, kc = queries.shape
    vc = values.shape[2]
    n = lax.axis_size("sa")
    half = heads // 2
    factor = (kc * lax.axis_size("ka")) ** -0.5
    dma = pltpu.SemaphoreType.DMA
    vmem = pl.BlockSpec(memory_space=pltpu.VMEM)
    narrow = jax.ShapeDtypeStruct((half, kc, rows), F32)
    wide = jax.ShapeDtypeStruct((rows * half, vc), F32)
    outs = pl.pallas_call(
        functools.partial(kernel, n, n // 2, factor),
        out_shape=(narrow, narrow, wide, narrow),
        in_specs=[pl.BlockSpec(memory_space=pltpu.HBM)] * 5,
        out_specs=(vmem,) * 4,
        scratch_shapes=[
            pltpu.VMEM((heads, kc, rows), BF16),
            pltpu.VMEM((heads, kc, rows), BF16),
            pltpu.VMEM((rows, heads, vc), BF16),
            pltpu.VMEM((heads, kc, rows), BF16),
            pltpu.VMEM((rows, heads, vc), BF16),
            pltpu.VMEM((rows * heads, vc), F32),
            pltpu.VMEM((rows * heads, vc), F32),
            pltpu.VMEM((heads, rows, vc), BF16),
            pltpu.VMEM((heads, rows, vc), BF16),
            pltpu.VMEM((heads, kc, 128), F32),
            pltpu.VMEM((heads, kc, 128), F32),
            pltpu.VMEM((heads, kc, rows), F32),
            pltpu.VMEM((heads, kc, rows), F32),
            pltpu.VMEM((heads, 2, kc, rows), F32),
            pltpu.VMEM((kc, 128), F32),
            pltpu.VMEM((kc, 128), F32),
            pltpu.VMEM((heads, 2, kc, vc), F32),
            pltpu.VMEM((heads, 2, kc, vc), F32),
            pltpu.VMEM((heads, kc, vc), F32),
            pltpu.VMEM((heads, kc, vc), F32),
            pltpu.VMEM((heads, kc, vc), F32),
            pltpu.VMEM((heads, kc, vc), F32),
            pltpu.VMEM((heads, 2, kc, vc), F32),
            pltpu.VMEM((heads, kc, vc), F32),
            pltpu.VMEM((heads, kc, vc), F32),
            pltpu.VMEM((heads, 3 * kc, rows), F32),
            pltpu.VMEM((half, 3 * kc, rows), F32),
            pltpu.VMEM((heads, rows, vc), F32),
            pltpu.VMEM((half, rows, vc), F32),
            dma((heads,)),
            dma((heads,)),
            dma((heads,)),
            dma((heads,)),
            dma((heads,)),
            dma((heads,)),
            dma((half,)),
            dma((half,)),
            dma((half,)),
            dma((half,)),
            dma,
            dma,
            dma((heads,)),
            dma((heads,)),
            dma((heads,)),
            dma((heads,)),
            dma((5,)),
        ],
        compiler_params=pltpu.CompilerParams(
            collective_id=0, has_side_effects=True, vmem_limit_bytes=67043328
        ),
    )(
        queries.transpose(1, 2, 0),
        key_rows.transpose(1, 2, 0),
        values,
        log_decays.transpose(1, 2, 0),
        output_grad,
    )
    query_grad, key_grad, value_grad, decay_grad = outs
    return (
        query_grad.transpose(2, 0, 1),
        key_grad.transpose(2, 0, 1),
        value_grad.reshape(rows, half, vc),
        decay_grad.transpose(2, 0, 1),
    )


def solution(mesh):
    return jax.shard_map(
        shards,
        mesh=mesh,
        in_specs=(
            P("sa", None, "ka"),
            P("sa", None, "ka"),
            P("sa", None, "vert"),
            P("sa", None, "ka"),
            P("sa", None, "vert"),
        ),
        out_specs=(
            P("sa", "vert", "ka"),
            P("sa", "vert", "ka"),
            P("sa", "ka", "vert"),
            P("sa", "vert", "ka"),
        ),
        check_vma=False,
    )
```

```python
import functools

import jax
import jax.numpy as jnp
from jax import lax
from jax.experimental import pallas as pl
from jax.experimental.pallas import tpu as pltpu
from jax.sharding import PartitionSpec as P

F32 = jnp.float32
BF16 = jnp.bfloat16
MESH = pl.DeviceIdType.MESH
LAG = 2

NN = (((1,), (0,)), ((), ()))
NT = (((1,), (1,)), ((), ()))
TN = (((0,), (0,)), ((), ()))


def mm(a, b, dims):
    return lax.dot_general(a, b, dims, preferred_element_type=F32)


def split(a):
    high = a.astype(BF16)
    return high, (a - high.astype(F32)).astype(BF16)


def kernel(
    n,
    pairs,
    factor,
    q_hbm,
    k_hbm,
    v_hbm,
    g_hbm,
    o_hbm,
    dq_ref,
    dk_ref,
    dv_ref,
    dg_ref,
    q_ref,
    k_ref,
    v_ref,
    g_ref,
    o_ref,
    vs,
    os,
    vb,
    ob,
    e_own,
    e_peer,
    grow,
    shrink,
    ends,
    decay,
    decay_in,
    own,
    peer,
    f_in,
    b_in,
    f_out,
    b_out,
    x_out,
    entry,
    leave,
    qk,
    qk_in,
    vg,
    vg_in,
    x_send,
    x_recv,
    f_send,
    f_recv,
    b_send,
    b_recv,
    q_send,
    q_recv,
    v_send,
    v_recv,
    d_send,
    d_recv,
    y_send,
    y_recv,
    w_send,
    w_recv,
    in_sem,
):
    heads, kc, rows = q_ref.shape
    vc = v_ref.shape[2]
    half = heads // 2
    quarter = half // 2
    loads = [
        pltpu.make_async_copy(source, target, in_sem.at[i])
        for i, (source, target) in enumerate(
            ((g_hbm, g_ref), (v_hbm, v_ref), (o_hbm, o_ref), (k_hbm, k_ref), (q_hbm, q_ref))
        )
    ]
    for load in loads:
        load.start()
    me = lax.axis_index("sa")
    ka = lax.axis_index("ka")
    vert = lax.axis_index("vert")
    pair = me // 2
    x = me % 2
    buddy = me + 1 - 2 * x
    first = pair == 0
    last = pair == pairs - 1

    barrier = pltpu.get_barrier_semaphore()

    def greet(where):
        pl.semaphore_signal(barrier, inc=1, device_id=where, device_id_type=MESH)

    greet({"sa": buddy})
    greet({"ka": 1 - ka})
    greet({"vert": 1 - vert})
    if pairs > 1:

        @pl.when(jnp.logical_not(first))
        def _():
            greet({"sa": me - 2})

        @pl.when(jnp.logical_not(last))
        def _():
            greet({"sa": me + 2})

    def remote(source, target, send, recv, where):
        return pltpu.make_async_remote_copy(
            src_ref=source,
            dst_ref=target,
            send_sem=send,
            recv_sem=recv,
            device_id=where,
            device_id_type=MESH,
        )

    def x_copy(h):
        return remote(own.at[h], peer.at[h], x_send.at[h], x_recv.at[h], {"sa": buddy})

    def y_copy(h):
        return remote(
            x_out.at[h, 0], peer.at[h, 0], y_send.at[h], y_recv.at[h], {"sa": buddy}
        )

    def w_copy(h):
        return remote(
            x_out.at[h, 1], peer.at[h, 1], w_send.at[h], w_recv.at[h], {"sa": buddy}
        )

    def d_copy():
        return remote(decay, decay_in, d_send, d_recv, {"sa": buddy})

    def f_copy(h):
        return remote(f_out.at[h], f_in.at[h], f_send.at[h], f_recv.at[h], {"sa": me + 2})

    def b_copy(h):
        return remote(b_out.at[h], b_in.at[h], b_send.at[h], b_recv.at[h], {"sa": me - 2})

    def q_copy(h, slot):
        return remote(qk.at[h], qk_in.at[slot], q_send.at[slot], q_recv.at[slot], {"vert": 1 - vert})

    def v_copy(h, slot):
        return remote(vg.at[h], vg_in.at[slot], v_send.at[slot], v_recv.at[slot], {"ka": 1 - ka})

    def first_set(j):
        return (j % 2) * half + j // 2

    def second_set(j):
        return first_set(j) + quarter

    def rows_of(h):
        return pl.ds(h, rows, stride=heads)

    ri = lax.broadcasted_iota(jnp.int32, (rows, rows), 0)
    ci = lax.broadcasted_iota(jnp.int32, (rows, rows), 1)
    lower = ri >= ci
    upper = ri <= ci
    upper_ones = upper.astype(F32).astype(BF16)
    lower_ones = lower.astype(F32).astype(BF16)
    lanes = lax.broadcasted_iota(jnp.int32, (kc, 128), 1)

    loads[0].wait()
    ones = jnp.ones((rows, 128), BF16)
    packed = jnp.zeros((kc, 128), F32)
    for h in range(heads):
        total = mm(g_ref[h], ones, NN)
        e_own[h] = jnp.exp(total)
        packed = jnp.where(lanes == h, total, packed)
    decay[...] = packed

    pl.semaphore_wait(
        barrier, 3 + (jnp.where(first, 0, 1) + jnp.where(last, 0, 1) if pairs > 1 else 0)
    )
    d_copy().start()

    for load in loads[1:]:
        load.wait()

    def stage(c, carry):
        for source, target in ((v_ref, vs), (o_ref, os)):
            piece = source[pl.ds(c * 8, 8)].astype(F32)
            target[pl.ds(pl.multiple_of(c * 8 * heads, 8 * heads), 8 * heads), :] = piece.reshape(
                8 * heads, source.shape[2]
            )
        return carry

    lax.fori_loop(0, rows // 8, stage, 0, unroll=4)

    mid = rows // 2 - 1

    def states(h):
        cum = mm(g_ref[h], upper_ones, NN)
        at_mid = cum[:, mid : mid + 1]
        at_end = cum[:, rows - 1 : rows]
        up = jnp.exp(cum - at_mid)
        down = jnp.exp(at_mid - cum)
        to_mid = jnp.exp(at_mid)
        to_end = jnp.exp(at_end - at_mid)
        grow[h] = up
        shrink[h] = down
        ends[h, 0] = jnp.broadcast_to(to_mid, (kc, rows))
        ends[h, 1] = jnp.broadcast_to(to_end, (kc, rows))
        key_high, key_low = split(k_ref[h].astype(F32) * (down * to_end))
        query_high, query_low = split(q_ref[h].astype(F32) * (up * to_mid) * factor)
        value = vs[rows_of(h), :].astype(BF16)
        cot = os[rows_of(h), :].astype(BF16)
        vb[h] = value
        ob[h] = cot
        own[h, 0] = mm(key_high, value, NN) + mm(key_low, value, NN)
        own[h, 1] = mm(query_high, cot, NN) + mm(query_low, cot, NN)

    def early(i, carry):
        for j in (2 * i, 2 * i + 1):
            states(first_set(j))
        for j in (2 * i, 2 * i + 1):
            x_copy(first_set(j)).start()
        return carry

    lax.fori_loop(0, quarter, early, 0)
    d_copy().wait_recv()
    received = decay_in[...]
    for h in range(heads):
        e_peer[h] = jnp.exp(jnp.broadcast_to(received[:, h : h + 1], (kc, 128)))

    def local(h):
        value = vb[h]
        cot = ob[h]
        key_high, key_low = split(k_ref[h].astype(F32) * shrink[h])
        query_high, query_low = split(q_ref[h].astype(F32) * grow[h] * factor)
        t_high, t_low = split(jnp.where(upper, mm(value, cot, NT), 0.0))
        qk[h, 0:kc] = mm(key_high, t_high, NN) + mm(key_low, t_high, NN) + mm(key_high, t_low, NN)
        s_high, s_low = split(jnp.where(lower, mm(cot, value, NT), 0.0))
        qk[h, kc : 2 * kc] = (
            mm(query_high, s_high, NN) + mm(query_low, s_high, NN) + mm(query_high, s_low, NN)
        )
        weights = (
            mm(key_high, query_high, TN) + mm(key_high, query_low, TN) + mm(key_low, query_high, TN)
        )
        w_high, w_low = split(jnp.where(upper, weights, 0.0))
        vg[h] = mm(w_high, cot, NN) + mm(w_low, cot, NN)

    def forward_pair(h):
        state = jnp.where(first, 0.0, f_in[h])
        arrived = jnp.where(x == 1, peer[h, 0] + e_peer[h] * state, state)
        entry[h] = arrived
        finish = e_own[h] * arrived + own[h, 0]
        f_out[h] = jnp.where(x == 1, finish, e_peer[h] * finish + peer[h, 0])

    def backward_pair(h):
        state = jnp.where(last, 0.0, b_in[h])
        arrived = jnp.where(x == 0, peer[h, 1] + e_peer[h] * state, state)
        leave[h] = arrived
        start = e_own[h] * arrived + own[h, 1]
        b_out[h] = jnp.where(x == 0, start, e_peer[h] * start + peer[h, 1])

    def forward_column(h):
        state = jnp.where(first, 0.0, f_in[h])
        finish = e_own[h] * state + own[h, 0]
        across = e_peer[h] * state
        entry[h] = jnp.where(x == 0, state, across)
        x_out[h, 0] = jnp.where(x == 0, finish, state)
        f_out[h] = jnp.where(x == 0, e_peer[h] * finish, e_own[h] * across + own[h, 0])

    def backward_column(h):
        state = jnp.where(last, 0.0, b_in[h])
        start = e_own[h] * state + own[h, 1]
        across = e_peer[h] * state
        leave[h] = jnp.where(x == 1, state, across)
        x_out[h, 1] = jnp.where(x == 1, start, state)
        b_out[h] = jnp.where(x == 1, e_peer[h] * start, e_own[h] * across + own[h, 1])

    def final(h, before, after):
        value = vb[h]
        cot = ob[h]
        to_mid = ends[h, 0]
        to_end = ends[h, 1]
        i_high, i_low = split(before)
        o_high, o_low = split(after)
        query_carried = mm(i_high, cot, NT) + mm(i_low, cot, NT)
        key_carried = mm(o_high, value, NT) + mm(o_low, value, NT)
        down = shrink[h]
        qk[h, 0:kc] = grow[h] * (qk[h, 0:kc] + to_mid * query_carried) * factor
        qk[h, kc : 2 * kc] = down * (qk[h, kc : 2 * kc] + to_end * key_carried)
        key_high, key_low = split(k_ref[h].astype(F32) * (down * to_end))
        vg[h] = vg[h] + (
            mm(key_high, o_high, TN) + mm(key_high, o_low, TN) + mm(key_low, o_high, TN)
        )
        crossing = (e_own[h] * before + own[h, 0]) * after
        beyond = jnp.sum(crossing, axis=1, keepdims=True)
        qk[h, 2 * kc : 3 * kc] = jnp.broadcast_to(beyond, (kc, rows))

    f_lag = LAG * pair
    b_lag = LAG * (pairs - 1 - pair)
    c_lag = jnp.maximum(f_lag, b_lag)
    second_lag = max(half, LAG * (pairs - 1) + 2)

    def forward_in(h):
        if pairs > 1:

            @pl.when(jnp.logical_not(first))
            def _():
                f_copy(h).wait_recv()

    def forward_on(h):
        if pairs > 1:

            @pl.when(jnp.logical_not(last))
            def _():
                f_copy(h).start()

    def backward_in(h):
        if pairs > 1:

            @pl.when(jnp.logical_not(last))
            def _():
                b_copy(h).wait_recv()

    def backward_on(h):
        if pairs > 1:

            @pl.when(jnp.logical_not(first))
            def _():
                b_copy(h).start()

    def send_parts(h):
        slot = h % half

        @pl.when(h // half != vert)
        def _():
            q_copy(h, slot).start()

        @pl.when(h // half != ka)
        def _():
            v_copy(h, slot).start()

    def inside(j):
        return jnp.logical_and(j >= 0, j < half)

    def step(t, carry):
        @pl.when(t < half)
        def _():
            states(second_set(t))
            local(first_set(t))
            x_copy(first_set(t)).wait_recv()

        @pl.when(inside(t - half))
        def _():
            local(second_set(t - half))

        fj = t - f_lag

        @pl.when(inside(fj))
        def _():
            column = second_set(fj)
            forward_in(column)
            forward_column(column)
            forward_on(column)
            y_copy(column).start()
            paired = first_set(fj)
            forward_in(paired)
            forward_pair(paired)
            forward_on(paired)

        bj = t - b_lag

        @pl.when(inside(bj))
        def _():
            column = second_set(bj)
            backward_in(column)
            backward_column(column)
            backward_on(column)
            w_copy(column).start()
            paired = first_set(bj)
            backward_in(paired)
            backward_pair(paired)
            backward_on(paired)

        cj = t - c_lag

        @pl.when(inside(cj))
        def _():
            h = first_set(cj)
            final(h, entry[h], leave[h])
            send_parts(h)

        sj = t - second_lag

        @pl.when(inside(sj))
        def _():
            h = second_set(sj)
            y_copy(h).wait_recv()
            w_copy(h).wait_recv()
            final(h, entry[h] + peer[h, 0], leave[h] + peer[h, 1])
            send_parts(h)

        return carry

    lax.fori_loop(0, half + second_lag, step, 0)

    def combine(i, carry):
        h = vert * half + i
        q_copy(h, i).wait_recv()
        query_grad = qk[h, 0:kc] + qk_in[i, 0:kc]
        key_grad = qk[h, kc : 2 * kc] + qk_in[i, kc : 2 * kc]
        dq_ref[i] = query_grad
        dk_ref[i] = key_grad
        position = q_ref[h].astype(F32) * query_grad - k_ref[h].astype(F32) * key_grad
        p_high, p_low = split(position)
        sums = mm(p_high, lower_ones, NN) + mm(p_low, lower_ones, NN)
        dg_ref[i] = sums + (qk[h, 2 * kc : 3 * kc] + qk_in[i, 2 * kc : 3 * kc])
        hv = ka * half + i
        v_copy(hv, i).wait_recv()
        dv_ref[pl.ds(i, rows, stride=half), :] = vg[hv] + vg_in[i]
        return carry

    lax.fori_loop(0, half, combine, 0)

    d_copy().wait_send()

    def drain(h, carry):
        if pairs > 1:

            @pl.when(jnp.logical_not(last))
            def _():
                f_copy(h).wait_send()

            @pl.when(jnp.logical_not(first))
            def _():
                b_copy(h).wait_send()

        return carry

    lax.fori_loop(0, heads, drain, 0)

    def drain_x(j, carry):
        x_copy(first_set(j)).wait_send()
        y_copy(second_set(j)).wait_send()
        w_copy(second_set(j)).wait_send()
        return carry

    lax.fori_loop(0, half, drain_x, 0)

    def drain_parts(i, carry):
        q_copy((1 - vert) * half + i, i).wait_send()
        v_copy((1 - ka) * half + i, i).wait_send()
        return carry

    lax.fori_loop(0, half, drain_parts, 0)


def place(*refs):
    copies = [
        pltpu.make_async_copy(refs[i], refs[4 + i], refs[8].at[i]) for i in (2, 0, 1, 3)
    ]
    for copy in copies:
        copy.start()
    for copy in copies:
        copy.wait()


def shards(queries, key_rows, values, log_decays, output_grad):
    rows, heads, kc = queries.shape
    vc = values.shape[2]
    n = lax.axis_size("sa")
    half = heads // 2
    factor = (kc * lax.axis_size("ka")) ** -0.5
    dma = pltpu.SemaphoreType.DMA
    vmem = pl.BlockSpec(memory_space=pltpu.VMEM)
    narrow = jax.ShapeDtypeStruct((half, kc, rows), F32)
    wide = jax.ShapeDtypeStruct((rows * half, vc), F32)
    outs = pl.pallas_call(
        functools.partial(kernel, n, n // 2, factor),
        out_shape=tuple(pltpu.VMEM(a.shape, a.dtype) for a in (narrow, narrow, wide, narrow)),
        in_specs=[pl.BlockSpec(memory_space=pltpu.HBM)] * 5,
        out_specs=(vmem,) * 4,
        scratch_shapes=[
            pltpu.VMEM((heads, kc, rows), BF16),
            pltpu.VMEM((heads, kc, rows), BF16),
            pltpu.VMEM((rows, heads, vc), BF16),
            pltpu.VMEM((heads, kc, rows), BF16),
            pltpu.VMEM((rows, heads, vc), BF16),
            pltpu.VMEM((rows * heads, vc), F32),
            pltpu.VMEM((rows * heads, vc), F32),
            pltpu.VMEM((heads, rows, vc), BF16),
            pltpu.VMEM((heads, rows, vc), BF16),
            pltpu.VMEM((heads, kc, 128), F32),
            pltpu.VMEM((heads, kc, 128), F32),
            pltpu.VMEM((heads, kc, rows), F32),
            pltpu.VMEM((heads, kc, rows), F32),
            pltpu.VMEM((heads, 2, kc, rows), F32),
            pltpu.VMEM((kc, 128), F32),
            pltpu.VMEM((kc, 128), F32),
            pltpu.VMEM((heads, 2, kc, vc), F32),
            pltpu.VMEM((heads, 2, kc, vc), F32),
            pltpu.VMEM((heads, kc, vc), F32),
            pltpu.VMEM((heads, kc, vc), F32),
            pltpu.VMEM((heads, kc, vc), F32),
            pltpu.VMEM((heads, kc, vc), F32),
            pltpu.VMEM((heads, 2, kc, vc), F32),
            pltpu.VMEM((heads, kc, vc), F32),
            pltpu.VMEM((heads, kc, vc), F32),
            pltpu.VMEM((heads, 3 * kc, rows), F32),
            pltpu.VMEM((half, 3 * kc, rows), F32),
            pltpu.VMEM((heads, rows, vc), F32),
            pltpu.VMEM((half, rows, vc), F32),
            dma((heads,)),
            dma((heads,)),
            dma((heads,)),
            dma((heads,)),
            dma((heads,)),
            dma((heads,)),
            dma((half,)),
            dma((half,)),
            dma((half,)),
            dma((half,)),
            dma,
            dma,
            dma((heads,)),
            dma((heads,)),
            dma((heads,)),
            dma((heads,)),
            dma((5,)),
        ],
        compiler_params=pltpu.CompilerParams(
            collective_id=0, has_side_effects=True, vmem_limit_bytes=65200128
        ),
    )(
        queries.transpose(1, 2, 0),
        key_rows.transpose(1, 2, 0),
        values,
        log_decays.transpose(1, 2, 0),
        output_grad,
    )
    query_grad, key_grad, value_grad, decay_grad = pl.pallas_call(
        place,
        out_shape=(narrow, narrow, wide, narrow),
        in_specs=[vmem] * 4,
        out_specs=(pl.BlockSpec(memory_space=pltpu.HBM),) * 4,
        scratch_shapes=[dma((4,))],
        compiler_params=pltpu.CompilerParams(vmem_limit_bytes=8 * 1024 * 1024),
    )(*outs)
    return (
        query_grad.transpose(2, 0, 1),
        key_grad.transpose(2, 0, 1),
        value_grad.reshape(rows, half, vc),
        decay_grad.transpose(2, 0, 1),
    )


def solution(mesh):
    return jax.shard_map(
        shards,
        mesh=mesh,
        in_specs=(
            P("sa", None, "ka"),
            P("sa", None, "ka"),
            P("sa", None, "vert"),
            P("sa", None, "ka"),
            P("sa", None, "vert"),
        ),
        out_specs=(
            P("sa", "vert", "ka"),
            P("sa", "vert", "ka"),
            P("sa", "ka", "vert"),
            P("sa", "vert", "ka"),
        ),
        check_vma=False,
    )
```

```python
import functools

import jax
import jax.numpy as jnp
from jax import lax
from jax.experimental import pallas as pl
from jax.experimental.pallas import tpu as pltpu
from jax.sharding import PartitionSpec as P

F32 = jnp.float32
BF16 = jnp.bfloat16
MESH = pl.DeviceIdType.MESH
LAG = 2

NN = (((1,), (0,)), ((), ()))
NT = (((1,), (1,)), ((), ()))
TN = (((0,), (0,)), ((), ()))


def mm(a, b, dims):
    return lax.dot_general(a, b, dims, preferred_element_type=F32)


def split(a):
    high = a.astype(BF16)
    return high, (a - high.astype(F32)).astype(BF16)


def kernel(
    n,
    pairs,
    factor,
    q_hbm,
    k_hbm,
    v_hbm,
    g_hbm,
    o_hbm,
    dq_ref,
    dk_ref,
    dv_ref,
    dg_ref,
    q_ref,
    k_ref,
    v_ref,
    g_ref,
    o_ref,
    vs,
    os,
    vb,
    ob,
    e_own,
    e_peer,
    grow,
    shrink,
    ends,
    decay,
    decay_in,
    own,
    peer,
    f_in,
    b_in,
    f_out,
    b_out,
    x_out,
    entry,
    leave,
    qk,
    qk_in,
    vg,
    vg_in,
    x_send,
    x_recv,
    f_send,
    f_recv,
    b_send,
    b_recv,
    q_send,
    q_recv,
    v_send,
    v_recv,
    d_send,
    d_recv,
    y_send,
    y_recv,
    w_send,
    w_recv,
    in_sem,
):
    heads, kc, rows = q_ref.shape
    vc = v_ref.shape[2]
    half = heads // 2
    quarter = half // 2
    loads = [
        pltpu.make_async_copy(source, target, in_sem.at[i])
        for i, (source, target) in enumerate(
            ((g_hbm, g_ref), (v_hbm, v_ref), (o_hbm, o_ref), (k_hbm, k_ref), (q_hbm, q_ref))
        )
    ]
    for load in loads:
        load.start()
    me = lax.axis_index("sa")
    ka = lax.axis_index("ka")
    vert = lax.axis_index("vert")
    pair = me // 2
    x = me % 2
    buddy = me + 1 - 2 * x
    first = pair == 0
    last = pair == pairs - 1

    barrier = pltpu.get_barrier_semaphore()

    def greet(where):
        pl.semaphore_signal(barrier, inc=1, device_id=where, device_id_type=MESH)

    greet({"sa": buddy})
    greet({"ka": 1 - ka})
    greet({"vert": 1 - vert})
    if pairs > 1:

        @pl.when(jnp.logical_not(first))
        def _():
            greet({"sa": me - 2})

        @pl.when(jnp.logical_not(last))
        def _():
            greet({"sa": me + 2})

    def remote(source, target, send, recv, where):
        return pltpu.make_async_remote_copy(
            src_ref=source,
            dst_ref=target,
            send_sem=send,
            recv_sem=recv,
            device_id=where,
            device_id_type=MESH,
        )

    def x_copy(h):
        return remote(own.at[h], peer.at[h], x_send.at[h], x_recv.at[h], {"sa": buddy})

    def y_copy(h):
        return remote(
            x_out.at[h, 0], peer.at[h, 0], y_send.at[h], y_recv.at[h], {"sa": buddy}
        )

    def w_copy(h):
        return remote(
            x_out.at[h, 1], peer.at[h, 1], w_send.at[h], w_recv.at[h], {"sa": buddy}
        )

    def d_copy():
        return remote(decay, decay_in, d_send, d_recv, {"sa": buddy})

    def f_copy(h):
        return remote(f_out.at[h], f_in.at[h], f_send.at[h], f_recv.at[h], {"sa": me + 2})

    def b_copy(h):
        return remote(b_out.at[h], b_in.at[h], b_send.at[h], b_recv.at[h], {"sa": me - 2})

    def q_copy(h, slot):
        return remote(qk.at[h], qk_in.at[slot], q_send.at[slot], q_recv.at[slot], {"vert": 1 - vert})

    def v_copy(h, slot):
        return remote(vg.at[h], vg_in.at[slot], v_send.at[slot], v_recv.at[slot], {"ka": 1 - ka})

    def first_set(j):
        return (j % 2) * half + j // 2

    def second_set(j):
        return first_set(j) + quarter

    def rows_of(h):
        return pl.ds(h, rows, stride=heads)

    ri = lax.broadcasted_iota(jnp.int32, (rows, rows), 0)
    ci = lax.broadcasted_iota(jnp.int32, (rows, rows), 1)
    lower = ri >= ci
    upper = ri <= ci
    upper_ones = upper.astype(F32).astype(BF16)
    lower_ones = lower.astype(F32).astype(BF16)
    lanes = lax.broadcasted_iota(jnp.int32, (kc, 128), 1)

    loads[0].wait()
    ones = jnp.ones((rows, 128), BF16)
    packed = jnp.zeros((kc, 128), F32)
    for h in range(heads):
        total = mm(g_ref[h], ones, NN)
        e_own[h] = jnp.exp(total)
        packed = jnp.where(lanes == h, total, packed)
    decay[...] = packed

    for load in loads[1:]:
        load.wait()

    def stage(c, carry):
        for source, target in ((v_ref, vs), (o_ref, os)):
            piece = source[pl.ds(c * 8, 8)].astype(F32)
            target[pl.ds(pl.multiple_of(c * 8 * heads, 8 * heads), 8 * heads), :] = piece.reshape(
                8 * heads, source.shape[2]
            )
        return carry

    lax.fori_loop(0, rows // 8, stage, 0, unroll=4)

    pl.semaphore_wait(
        barrier, 3 + (jnp.where(first, 0, 1) + jnp.where(last, 0, 1) if pairs > 1 else 0)
    )
    d_copy().start()

    mid = rows // 2 - 1

    def states(h):
        cum = mm(g_ref[h], upper_ones, NN)
        at_mid = cum[:, mid : mid + 1]
        at_end = cum[:, rows - 1 : rows]
        up = jnp.exp(cum - at_mid)
        down = jnp.exp(at_mid - cum)
        to_mid = jnp.exp(at_mid)
        to_end = jnp.exp(at_end - at_mid)
        grow[h] = up
        shrink[h] = down
        ends[h, 0] = jnp.broadcast_to(to_mid, (kc, rows))
        ends[h, 1] = jnp.broadcast_to(to_end, (kc, rows))
        key_high, key_low = split(k_ref[h].astype(F32) * (down * to_end))
        query_high, query_low = split(q_ref[h].astype(F32) * (up * to_mid) * factor)
        value = vs[rows_of(h), :].astype(BF16)
        cot = os[rows_of(h), :].astype(BF16)
        vb[h] = value
        ob[h] = cot
        own[h, 0] = mm(key_high, value, NN) + mm(key_low, value, NN)
        own[h, 1] = mm(query_high, cot, NN) + mm(query_low, cot, NN)

    def early(i, carry):
        for j in (2 * i, 2 * i + 1):
            states(first_set(j))
        for j in (2 * i, 2 * i + 1):
            x_copy(first_set(j)).start()
        return carry

    lax.fori_loop(0, quarter, early, 0)
    d_copy().wait_recv()
    received = decay_in[...]
    for h in range(heads):
        e_peer[h] = jnp.exp(jnp.broadcast_to(received[:, h : h + 1], (kc, 128)))

    def local(h):
        value = vb[h]
        cot = ob[h]
        key_high, key_low = split(k_ref[h].astype(F32) * shrink[h])
        query_high, query_low = split(q_ref[h].astype(F32) * grow[h] * factor)
        t_high, t_low = split(jnp.where(upper, mm(value, cot, NT), 0.0))
        qk[h, 0:kc] = mm(key_high, t_high, NN) + mm(key_low, t_high, NN) + mm(key_high, t_low, NN)
        s_high, s_low = split(jnp.where(lower, mm(cot, value, NT), 0.0))
        qk[h, kc : 2 * kc] = (
            mm(query_high, s_high, NN) + mm(query_low, s_high, NN) + mm(query_high, s_low, NN)
        )
        weights = (
            mm(key_high, query_high, TN) + mm(key_high, query_low, TN) + mm(key_low, query_high, TN)
        )
        w_high, w_low = split(jnp.where(upper, weights, 0.0))
        vg[h] = mm(w_high, cot, NN) + mm(w_low, cot, NN)

    def forward_pair(h):
        state = jnp.where(first, 0.0, f_in[h])
        arrived = jnp.where(x == 1, peer[h, 0] + e_peer[h] * state, state)
        entry[h] = arrived
        finish = e_own[h] * arrived + own[h, 0]
        f_out[h] = jnp.where(x == 1, finish, e_peer[h] * finish + peer[h, 0])

    def backward_pair(h):
        state = jnp.where(last, 0.0, b_in[h])
        arrived = jnp.where(x == 0, peer[h, 1] + e_peer[h] * state, state)
        leave[h] = arrived
        start = e_own[h] * arrived + own[h, 1]
        b_out[h] = jnp.where(x == 0, start, e_peer[h] * start + peer[h, 1])

    def forward_column(h):
        state = jnp.where(first, 0.0, f_in[h])
        finish = e_own[h] * state + own[h, 0]
        across = e_peer[h] * state
        entry[h] = jnp.where(x == 0, state, across)
        x_out[h, 0] = jnp.where(x == 0, finish, state)
        f_out[h] = jnp.where(x == 0, e_peer[h] * finish, e_own[h] * across + own[h, 0])

    def backward_column(h):
        state = jnp.where(last, 0.0, b_in[h])
        start = e_own[h] * state + own[h, 1]
        across = e_peer[h] * state
        leave[h] = jnp.where(x == 1, state, across)
        x_out[h, 1] = jnp.where(x == 1, start, state)
        b_out[h] = jnp.where(x == 1, e_peer[h] * start, e_own[h] * across + own[h, 1])

    def final(h, before, after):
        value = vb[h]
        cot = ob[h]
        to_mid = ends[h, 0]
        to_end = ends[h, 1]
        i_high, i_low = split(before)
        o_high, o_low = split(after)
        query_carried = mm(i_high, cot, NT) + mm(i_low, cot, NT)
        key_carried = mm(o_high, value, NT) + mm(o_low, value, NT)
        down = shrink[h]
        qk[h, 0:kc] = grow[h] * (qk[h, 0:kc] + to_mid * query_carried) * factor
        qk[h, kc : 2 * kc] = down * (qk[h, kc : 2 * kc] + to_end * key_carried)
        key_high, key_low = split(k_ref[h].astype(F32) * (down * to_end))
        vg[h] = vg[h] + (
            mm(key_high, o_high, TN) + mm(key_high, o_low, TN) + mm(key_low, o_high, TN)
        )
        crossing = (e_own[h] * before + own[h, 0]) * after
        beyond = jnp.sum(crossing, axis=1, keepdims=True)
        qk[h, 2 * kc : 3 * kc] = jnp.broadcast_to(beyond, (kc, rows))

    f_lag = LAG * pair
    b_lag = LAG * (pairs - 1 - pair)
    c_lag = jnp.maximum(f_lag, b_lag)
    second_lag = max(half, LAG * (pairs - 1) + 2)

    def forward_in(h):
        if pairs > 1:

            @pl.when(jnp.logical_not(first))
            def _():
                f_copy(h).wait_recv()

    def forward_on(h):
        if pairs > 1:

            @pl.when(jnp.logical_not(last))
            def _():
                f_copy(h).start()

    def backward_in(h):
        if pairs > 1:

            @pl.when(jnp.logical_not(last))
            def _():
                b_copy(h).wait_recv()

    def backward_on(h):
        if pairs > 1:

            @pl.when(jnp.logical_not(first))
            def _():
                b_copy(h).start()

    def send_parts(h):
        slot = h % half

        @pl.when(h // half != vert)
        def _():
            q_copy(h, slot).start()

        @pl.when(h // half != ka)
        def _():
            v_copy(h, slot).start()

    def inside(j):
        return jnp.logical_and(j >= 0, j < half)

    def step(t, carry):
        @pl.when(t < half)
        def _():
            states(second_set(t))
            local(first_set(t))
            x_copy(first_set(t)).wait_recv()

        @pl.when(inside(t - half))
        def _():
            local(second_set(t - half))

        fj = t - f_lag

        @pl.when(inside(fj))
        def _():
            column = second_set(fj)
            forward_in(column)
            forward_column(column)
            forward_on(column)
            y_copy(column).start()
            paired = first_set(fj)
            forward_in(paired)
            forward_pair(paired)
            forward_on(paired)

        bj = t - b_lag

        @pl.when(inside(bj))
        def _():
            column = second_set(bj)
            backward_in(column)
            backward_column(column)
            backward_on(column)
            w_copy(column).start()
            paired = first_set(bj)
            backward_in(paired)
            backward_pair(paired)
            backward_on(paired)

        cj = t - c_lag

        @pl.when(inside(cj))
        def _():
            h = first_set(cj)
            final(h, entry[h], leave[h])
            send_parts(h)

        sj = t - second_lag

        @pl.when(inside(sj))
        def _():
            h = second_set(sj)
            y_copy(h).wait_recv()
            w_copy(h).wait_recv()
            final(h, entry[h] + peer[h, 0], leave[h] + peer[h, 1])
            send_parts(h)

        return carry

    lax.fori_loop(0, half + second_lag, step, 0)

    def combine(i, carry):
        h = vert * half + i
        q_copy(h, i).wait_recv()
        query_grad = qk[h, 0:kc] + qk_in[i, 0:kc]
        key_grad = qk[h, kc : 2 * kc] + qk_in[i, kc : 2 * kc]
        dq_ref[i] = query_grad
        dk_ref[i] = key_grad
        position = q_ref[h].astype(F32) * query_grad - k_ref[h].astype(F32) * key_grad
        p_high, p_low = split(position)
        sums = mm(p_high, lower_ones, NN) + mm(p_low, lower_ones, NN)
        dg_ref[i] = sums + (qk[h, 2 * kc : 3 * kc] + qk_in[i, 2 * kc : 3 * kc])
        hv = ka * half + i
        v_copy(hv, i).wait_recv()
        dv_ref[pl.ds(i, rows, stride=half), :] = vg[hv] + vg_in[i]
        return carry

    lax.fori_loop(0, half, combine, 0)

    d_copy().wait_send()

    def drain(h, carry):
        if pairs > 1:

            @pl.when(jnp.logical_not(last))
            def _():
                f_copy(h).wait_send()

            @pl.when(jnp.logical_not(first))
            def _():
                b_copy(h).wait_send()

        return carry

    lax.fori_loop(0, heads, drain, 0)

    def drain_x(j, carry):
        x_copy(first_set(j)).wait_send()
        y_copy(second_set(j)).wait_send()
        w_copy(second_set(j)).wait_send()
        return carry

    lax.fori_loop(0, half, drain_x, 0)

    def drain_parts(i, carry):
        q_copy((1 - vert) * half + i, i).wait_send()
        v_copy((1 - ka) * half + i, i).wait_send()
        return carry

    lax.fori_loop(0, half, drain_parts, 0)


def place(*refs):
    copies = [
        pltpu.make_async_copy(refs[i], refs[4 + i], refs[8].at[i]) for i in (2, 0, 1, 3)
    ]
    for copy in copies:
        copy.start()
    for copy in copies:
        copy.wait()


def shards(queries, key_rows, values, log_decays, output_grad):
    rows, heads, kc = queries.shape
    vc = values.shape[2]
    n = lax.axis_size("sa")
    half = heads // 2
    factor = (kc * lax.axis_size("ka")) ** -0.5
    dma = pltpu.SemaphoreType.DMA
    vmem = pl.BlockSpec(memory_space=pltpu.VMEM)
    narrow = jax.ShapeDtypeStruct((half, kc, rows), F32)
    wide = jax.ShapeDtypeStruct((rows * half, vc), F32)
    outs = pl.pallas_call(
        functools.partial(kernel, n, n // 2, factor),
        out_shape=tuple(pltpu.VMEM(a.shape, a.dtype) for a in (narrow, narrow, wide, narrow)),
        in_specs=[pl.BlockSpec(memory_space=pltpu.HBM)] * 5,
        out_specs=(vmem,) * 4,
        scratch_shapes=[
            pltpu.VMEM((heads, kc, rows), BF16),
            pltpu.VMEM((heads, kc, rows), BF16),
            pltpu.VMEM((rows, heads, vc), BF16),
            pltpu.VMEM((heads, kc, rows), BF16),
            pltpu.VMEM((rows, heads, vc), BF16),
            pltpu.VMEM((rows * heads, vc), F32),
            pltpu.VMEM((rows * heads, vc), F32),
            pltpu.VMEM((heads, rows, vc), BF16),
            pltpu.VMEM((heads, rows, vc), BF16),
            pltpu.VMEM((heads, kc, 128), F32),
            pltpu.VMEM((heads, kc, 128), F32),
            pltpu.VMEM((heads, kc, rows), F32),
            pltpu.VMEM((heads, kc, rows), F32),
            pltpu.VMEM((heads, 2, kc, rows), F32),
            pltpu.VMEM((kc, 128), F32),
            pltpu.VMEM((kc, 128), F32),
            pltpu.VMEM((heads, 2, kc, vc), F32),
            pltpu.VMEM((heads, 2, kc, vc), F32),
            pltpu.VMEM((heads, kc, vc), F32),
            pltpu.VMEM((heads, kc, vc), F32),
            pltpu.VMEM((heads, kc, vc), F32),
            pltpu.VMEM((heads, kc, vc), F32),
            pltpu.VMEM((heads, 2, kc, vc), F32),
            pltpu.VMEM((heads, kc, vc), F32),
            pltpu.VMEM((heads, kc, vc), F32),
            pltpu.VMEM((heads, 3 * kc, rows), F32),
            pltpu.VMEM((half, 3 * kc, rows), F32),
            pltpu.VMEM((heads, rows, vc), F32),
            pltpu.VMEM((half, rows, vc), F32),
            dma((heads,)),
            dma((heads,)),
            dma((heads,)),
            dma((heads,)),
            dma((heads,)),
            dma((heads,)),
            dma((half,)),
            dma((half,)),
            dma((half,)),
            dma((half,)),
            dma,
            dma,
            dma((heads,)),
            dma((heads,)),
            dma((heads,)),
            dma((heads,)),
            dma((5,)),
        ],
        compiler_params=pltpu.CompilerParams(
            collective_id=0, has_side_effects=True, vmem_limit_bytes=65200128
        ),
    )(
        queries.transpose(1, 2, 0),
        key_rows.transpose(1, 2, 0),
        values,
        log_decays.transpose(1, 2, 0),
        output_grad,
    )
    query_grad, key_grad, value_grad, decay_grad = pl.pallas_call(
        place,
        out_shape=(narrow, narrow, wide, narrow),
        in_specs=[vmem] * 4,
        out_specs=(pl.BlockSpec(memory_space=pltpu.HBM),) * 4,
        scratch_shapes=[dma((4,))],
        compiler_params=pltpu.CompilerParams(vmem_limit_bytes=8 * 1024 * 1024),
    )(*outs)
    return (
        query_grad.transpose(2, 0, 1),
        key_grad.transpose(2, 0, 1),
        value_grad.reshape(rows, half, vc),
        decay_grad.transpose(2, 0, 1),
    )


def solution(mesh):
    return jax.shard_map(
        shards,
        mesh=mesh,
        in_specs=(
            P("sa", None, "ka"),
            P("sa", None, "ka"),
            P("sa", None, "vert"),
            P("sa", None, "ka"),
            P("sa", None, "vert"),
        ),
        out_specs=(
            P("sa", "vert", "ka"),
            P("sa", "vert", "ka"),
            P("sa", "ka", "vert"),
            P("sa", "vert", "ka"),
        ),
        check_vma=False,
    )
```
